32 devices in a mesh: ea: 4 (over y, x), row: 4 (over z), col: 2 (over core).
Axes of the slice: x: 2, y: 2, z: 4, core: 2. Of those that a mesh axis runs over, the one named last changes fastest.
Arguments:
- weights: float32 [4, 256, 2048], P('ea', 'row', 'col'), parts along dimension 0, may hold values from -6 to 6
- codebook: float32 [4, 16, 2, 256], P('ea', 'col'), parts along dimension 0, may hold values from -4 to 4
- assign: int32 [4, 256, 1024], P('ea', 'row', 'col'), parts along dimension 0, may hold values from 0 to 255
- chol_upper: float32 [4, 2048, 2048], P('ea', 'row', 'col'), parts along dimension 0, may hold values from 0 to 1.4, as said below
- inv_blocks: float32 [4, 16, 128, 128], P('ea', 'col'), parts along dimension 0, may hold values from -1 to 1.5, as said below
Outputs:
- errors: float32 [4, 256, 2048], P('ea', 'row', 'col'), parts along dimension 0
- row_loss: float32 [4, 256], P('ea', 'row'), parts along dimension 0
- codeword_mass: float32 [4, 16, 256], P('ea', 'col'), parts along dimension 0
The draws below stay inside these ranges and needn't reach their ends.
There are 4 independent parts, one for each index of `ea`. The reference program is written for one: setup_inputs(seed, part) draws one part's arguments, and reference() takes and returns one part's arrays. A program takes and returns all parts, laid end to end along the dimension named above; each array names one. Nothing has to cross between parts.
Inputs may be any that keep to these rules, and one draw needn't show every extreme that they name: `chol_upper`: upper triangular with a positive diagonal. inv_blocks[x, b] is the inverse of the diagonal block of chol_upper[x] on rows and columns [b * 128, (b + 1) * 128).
All inputs are finite; a program needn't handle non-finite values.
Results may differ from the reference program's by a relative error of at most 0.0001.
Values sent between devices are 32-bit elements; how exact they have to be, the bound alone decides.
A program may use at most 64 MiB of HBM per device.

```python
import jax
import jax.numpy as jnp
from jax import lax

EXP_PART = 1
COLS = 2048
BLOCK = 128
CODES = 256
ROWS = 256
NBLK = 16


def upper_factor(key):
    folded = jax.random.fold_in(key, 7)
    key_diag, key_near, key_far = jax.random.split(folded, 3)
    diagonal = jax.random.uniform(key_diag, (EXP_PART, COLS), jnp.float32, 0.7, 1.4)
    near_part = jax.random.uniform(key_near, (EXP_PART, COLS, COLS), jnp.float32, 0.0, 0.03)
    far_part = jax.random.uniform(key_far, (EXP_PART, COLS, COLS), jnp.float32, 0.0, 0.03)
    positions = jnp.arange(COLS, dtype=jnp.int32)
    same_block = positions[:, None] // BLOCK == positions[None, :] // BLOCK
    strictly_upper = positions[:, None] < positions[None, :]
    offdiag = jnp.where(same_block[None], near_part, far_part) * strictly_upper[None].astype(jnp.float32)
    return offdiag + diagonal[:, :, None] * jnp.eye(COLS, dtype=jnp.float32)[None]


def draw_chol_upper(key, part):
    return upper_factor(key)


def draw_inv_blocks(key, part):
    factor = upper_factor(key)
    blocked = factor.reshape(EXP_PART, NBLK, BLOCK, NBLK, BLOCK)
    which = jnp.arange(NBLK, dtype=jnp.int32)
    diagonal_blocks = jnp.transpose(blocked[:, which, :, which, :], (1, 0, 2, 3))
    return jnp.linalg.inv(diagonal_blocks)


def place_ends(array, key, smallest, high):
    shape = array.shape
    place = [jax.random.randint(jax.random.fold_in(key, axis), (), 0, shape[axis]) for axis in range(len(shape))]
    array = array.at[tuple(place)].set(smallest)
    longest = shape.index(max(shape))
    place[longest] = (place[longest] + 1) % shape[longest]
    return array.at[tuple(place)].set(high)


def levels(stream_key, shape, cuts, least, top_value):
    gain, own = 1.0, jax.random.fold_in(stream_key, 6)
    for axis_at, blocks in cuts:
        draws = jnp.exp(jax.random.uniform(jax.random.fold_in(own, axis_at), (blocks,), jnp.float32, least / len(cuts), top_value / len(cuts)))
        gain = gain * jnp.repeat(draws, shape[axis_at] // blocks).reshape([-1 if axis == axis_at else 1 for axis in range(len(shape))])
    return gain


def gaussian(key, dims, width, bound, shards=(), kind=jnp.bfloat16):
    drawn = width * jax.random.normal(key, dims, jnp.float32)
    if shards:
        drawn = drawn * levels(key, dims, shards, -0.22, 0.18)
    return jnp.clip(drawn, -bound, bound).astype(kind)


def setup_inputs(seed: int = 0, part: int = 0) -> dict:
    key_of = jax.random.split(jax.random.key(seed), 6)
    own_keys = jax.random.split(jax.random.fold_in(key_of[5], part), 6)
    weights = gaussian(own_keys[0], (EXP_PART, ROWS, COLS), 1.0, 6.0, ((1, 4), (2, 2)), jnp.float32)
    codebook = gaussian(own_keys[1], (EXP_PART, NBLK, 2, CODES), 1.0, 4.0, ((1, 2),), jnp.float32)
    assign = place_ends(jax.random.randint(own_keys[2], (EXP_PART, ROWS, COLS // 2), 0, CODES), jax.random.fold_in(own_keys[2], 1), 0, CODES - 1).astype(jnp.int32)
    chol_upper = draw_chol_upper(jax.random.fold_in(jax.random.fold_in(key_of[5], part), 71), part)
    inv_blocks = draw_inv_blocks(jax.random.fold_in(jax.random.fold_in(key_of[5], part), 71), part)
    return {"weights": weights, "codebook": codebook, "assign": assign, "chol_upper": chol_upper, "inv_blocks": inv_blocks}


def lookup(codebook, assign, half_block, code_count):
    pair_count = assign.shape[2]
    offsets = jnp.arange(pair_count, dtype=jnp.int32) // half_block * code_count
    flat_index = (assign + offsets[None, None, :]).astype(jnp.int32)
    experts = codebook.shape[0]
    code_table = jnp.transpose(codebook, (0, 2, 1, 3)).reshape(experts, 2, -1)

    def select(rows_table, indices):
        return jnp.stack([jnp.take(rows_table[0], indices), jnp.take(rows_table[1], indices)], axis=-1)
    picked = jax.vmap(select)(code_table, flat_index)
    return (picked.reshape(assign.shape[0], assign.shape[1], 2 * pair_count), flat_index)

def mass_by_code(errors, flat_index, segments):
    squared = errors * errors
    extent = errors.shape
    paired = squared.reshape(extent[0], extent[1], extent[2] // 2, 2).sum(axis=3)

    def summed(values, labels):
        return jax.ops.segment_sum(values.reshape(-1), labels.reshape(-1), num_segments=segments)
    return jax.vmap(summed)(paired, flat_index)

def reference(weights, codebook, assign, chol_upper, inv_blocks):
    quantized, flat_index = lookup(codebook, assign, BLOCK // 2, CODES)
    current = weights
    pieces = []
    for number in range(NBLK):
        first_col = number * BLOCK
        finish = first_col + BLOCK
        error_block = jnp.einsum('xrc,xcd->xrd', current[:, :, first_col:finish] - quantized[:, :, first_col:finish], inv_blocks[:, number], precision=lax.Precision.HIGHEST)
        pieces.append(error_block)
        if finish < COLS:
            change = jnp.einsum('xrc,xcd->xrd', error_block, chol_upper[:, first_col:finish, finish:], precision=lax.Precision.HIGHEST)
            current = jnp.concatenate([current[:, :, :finish], current[:, :, finish:] - change], axis=2)
    errors = jnp.concatenate(pieces, axis=2)
    row_loss = jnp.sum(errors * errors, axis=2)
    codeword_mass = mass_by_code(errors, flat_index, NBLK * CODES).reshape(EXP_PART, NBLK, CODES)
    return (errors, row_loss, codeword_mass)
```

```python
import functools

import jax
import jax.numpy as jnp
from jax import lax
from jax.experimental import pallas as pl
from jax.experimental.pallas import tpu as pltpu
from jax.sharding import PartitionSpec as P

F32 = jnp.float32
BF16 = jnp.bfloat16
LOW = 16


def halves(value):
    high = value.astype(BF16)
    return high, (value - high.astype(F32)).astype(BF16)


def dot(a, b):
    return jnp.dot(a, b, preferred_element_type=F32)


def dot3(a, b_high, b_low):
    rows = a.shape[0]
    high, low = halves(a)
    both = dot(jnp.concatenate([high, low], axis=0), b_high)
    return both[:rows] + both[rows:] + dot(high, b_low)


def dot_full(a, b):
    b_high, b_low = halves(b)
    return dot3(a, b_high, b_low)


def take(table, index):
    return jnp.take_along_axis(table, index, axis=1, mode="promise_in_bounds")


def kernel(
    nr, nc,
    weights, codebook, assign, inverse, factor,
    errors_out, loss_out, mass_out,
    u_raw, u_high, u_low, v_full, v_high, v_low, delta, codes, delta_in, run_in, run_out,
    err_block, err_own, mass_all, loss_all,
    u_sem, d_send, d_recv, run_send, run_recv, core_send, core_recv, own_send, own_recv,
    mass_send, mass_recv, loss_send, loss_recv,
):
    z = lax.axis_index("row")
    c = lax.axis_index("col")
    rows, width = weights.shape
    span = factor.shape[0]
    m = width // span
    block = inverse.shape[1]
    k = span // block
    code_count = codebook.shape[2]
    owner = z // m
    slot = z % m
    is_owner = c == owner

    def remote(src, dst, send, recv, row, col):
        return pltpu.make_async_remote_copy(
            src_ref=src, dst_ref=dst, send_sem=send, recv_sem=recv,
            device_id={"row": row, "col": col}, device_id_type=pl.DeviceIdType.MESH,
        )

    load = pltpu.make_async_copy(factor, u_raw, u_sem)
    load.start()

    barrier = pltpu.get_barrier_semaphore()
    for step in range(1, nr * nc):
        other = lax.rem(z * nc + c + step, nr * nc)
        pl.semaphore_signal(
            barrier, inc=1, device_id={"row": other // nc, "col": other % nc},
            device_id_type=pl.DeviceIdType.MESH,
        )

    lane = lax.broadcasted_iota(jnp.int32, (rows, block), 1)
    for b in range(width // block):
        first = b * (block // 2)
        tile = first // block * block
        code = take(assign[:, tile:tile + block], first - tile + lane // 2)
        codes[b] = code
        inner = code % block
        value = jnp.zeros((rows, block), F32)
        for part in range(code_count // block):
            picked = []
            for comp in range(2):
                table = codebook[b, comp:comp + 1, part * block:(part + 1) * block]
                picked.append(take(jnp.broadcast_to(table, (rows, block)), inner))
            both = jnp.where(lane % 2 == 0, picked[0], picked[1])
            value = jnp.where(code // block == part, both, value)
        j, at = b * block // span, b * block % span
        delta[j, :, at:at + block] = weights[:, b * block:(b + 1) * block] - value

    @pl.when(z == 0)
    def _():
        run_in[...] = jnp.zeros_like(run_in)

    pl.semaphore_wait(barrier, nr * nc - 1)

    def delta_copy(j):
        return remote(delta.at[j], delta_in.at[z], d_send.at[j], d_recv.at[z], c * m + j, c)

    for j in range(m):
        @pl.when(c * m + j < z)
        def _():
            delta_copy(j).start()

    load.wait()

    @pl.when(is_owner)
    def _():
        v_full[...] = jnp.zeros_like(v_full)
        base = slot * span

        def invert(lo, hi):
            if hi - lo == 1:
                v_full[lo * block:hi * block, lo * block:hi * block] = inverse[slot * k + lo]
                return
            mid = (lo + hi) // 2
            invert(lo, mid)
            invert(mid, hi)
            top, middle, end = lo * block, mid * block, hi * block
            right = u_raw[top:middle, pl.ds(pl.multiple_of(base + middle, block), end - middle)]
            product = dot_full(v_full[top:middle, top:middle], right)
            v_full[top:middle, middle:end] = -dot_full(product, v_full[middle:end, middle:end])

        invert(0, k)
        high, low = halves(v_full[...])
        v_high[...] = high
        v_low[...] = low

    for j in range(m):
        @pl.when(c * m + j > z)
        def _():
            high, low = halves(u_raw[:, j * span:(j + 1) * span])
            u_high[:, j * span:(j + 1) * span] = high
            u_low[:, j * span:(j + 1) * span] = low

    def run_copy(g, j):
        return remote(run_out.at[g, j], run_in.at[g, j], run_send.at[g, j], run_recv.at[g, j], z + 1, c)

    def core_copy(g, col):
        return remote(err_block.at[g], err_block.at[g], core_send.at[g, col], core_recv.at[g], z, col)

    def own_copy(g):
        return remote(err_block.at[g], err_own.at[slot], own_send.at[g], own_recv.at[slot], g, c)

    def arrived(ref, sem):
        pltpu.make_async_copy(ref, ref, sem).wait()

    def stage(g, _):
        @pl.when(is_owner)
        def _():
            @pl.when(z > 0)
            def _():
                arrived(run_in.at[g, slot], run_recv.at[g, slot])

            @pl.when(g > z)
            def _():
                arrived(delta_in.at[g], d_recv.at[g])
                run_in[g, slot] = run_in[g, slot] + delta_in[g]

            @pl.when(g == z)
            def _():
                run_in[g, slot] = run_in[g, slot] + delta[slot]

            error = dot3(run_in[g, slot], v_high[...], v_low[...])
            err_block[g] = error

            @pl.when(g == z)
            def _():
                err_own[slot] = error

            for col in range(1, nc):
                @pl.when(col > c)
                def _():
                    core_copy(g, col).start()

            @pl.when(g != z)
            def _():
                own_copy(g).start()

        @pl.when(c > owner)
        def _():
            arrived(err_block.at[g], core_recv.at[g])

        for j in range(m):
            @pl.when(c * m + j > z)
            def _():
                change = dot3(
                    err_block[g], u_high[:, j * span:(j + 1) * span], u_low[:, j * span:(j + 1) * span]
                )

                @pl.when(z > 0)
                def _():
                    arrived(run_in.at[g, j], run_recv.at[g, j])

                local = jnp.where(g == z, delta[j], 0.0)
                run_out[g, j] = run_in[g, j] + local - change
                run_copy(g, j).start()

        return 0

    lax.fori_loop(0, nr, stage, 0)

    high_count = code_count // LOW
    group = 2 * high_count
    chunk = 8
    loss = jnp.zeros((8, rows), F32)
    for j in range(m):
        @pl.when(c * m + j != z)
        def _():
            arrived(err_own.at[j], own_recv.at[j])

        error = err_own[j]
        errors_out[:, j * span:(j + 1) * span] = error
        squared = error * error
        loss = loss + lax.dot_general(
            jnp.ones((8, span), F32), squared, (((1,), (1,)), ((), ())),
            precision=lax.Precision.HIGHEST, preferred_element_type=F32,
        )

        def gather(step, total):
            at = pl.ds(pl.multiple_of(step * chunk, chunk), chunk)
            iota_high = lax.broadcasted_iota(jnp.int32, (high_count, block), 0)
            iota_low = lax.broadcasted_iota(jnp.int32, (LOW, block), 0)
            left, right = [], []
            for b in range(k):
                code = codes[j * k + b, at, :]
                value = err_own[j, at, b * block:(b + 1) * block]
                value = value * value
                coarse = value.astype(BF16).astype(F32)
                fine = value - coarse
                code_high, code_low = code // LOW, code % LOW
                top, bottom, marks = [], [], []
                for r in range(chunk):
                    hit = jnp.broadcast_to(code_high[r:r + 1], (high_count, block)) == iota_high
                    top.append(jnp.where(hit, jnp.broadcast_to(coarse[r:r + 1], (high_count, block)), 0.0).astype(BF16))
                    bottom.append(jnp.where(hit, jnp.broadcast_to(fine[r:r + 1], (high_count, block)), 0.0).astype(BF16))
                    low_hit = jnp.broadcast_to(code_low[r:r + 1], (LOW, block)) == iota_low
                    marks.append(jnp.where(low_hit, 1.0, 0.0).astype(BF16))
                left += [jnp.concatenate(top, axis=1), jnp.concatenate(bottom, axis=1)]
                right.append(jnp.concatenate(marks, axis=1))
            return total + lax.dot_general(
                jnp.concatenate(left, axis=0), jnp.concatenate(right, axis=0),
                (((1,), (1,)), ((), ())), preferred_element_type=F32,
            )

        total = lax.fori_loop(0, rows // chunk, gather, jnp.zeros((k * group, k * LOW), F32))
        row_id = lax.broadcasted_iota(jnp.int32, total.shape, 0)
        col_id = lax.broadcasted_iota(jnp.int32, total.shape, 1)
        total = jnp.where(row_id // group == col_id // LOW, total, 0.0)
        wide_row = lax.broadcasted_iota(jnp.int32, (k * LOW, code_count), 0)
        wide_col = lax.broadcasted_iota(jnp.int32, (k * LOW, code_count), 1)
        spread = jnp.where(wide_row % LOW == wide_col % LOW, 1.0, 0.0)
        spread = jnp.dot(total, spread, precision=lax.Precision.HIGHEST, preferred_element_type=F32)
        out_row = lax.broadcasted_iota(jnp.int32, spread.shape, 0)
        out_col = lax.broadcasted_iota(jnp.int32, spread.shape, 1)
        spread = jnp.where(out_row % high_count == out_col // LOW, spread, 0.0)
        for b in range(k):
            mass_all[z, j * k + b:j * k + b + 1, :] = jnp.sum(
                spread[b * group:(b + 1) * group], axis=0, keepdims=True
            )

    loss_all[c, :, :rows] = loss

    def mass_copy(row):
        return remote(mass_all.at[z], mass_all.at[z], mass_send.at[row], mass_recv.at[z], row, c)

    def loss_copy(col):
        return remote(loss_all.at[c], loss_all.at[c], loss_send.at[col], loss_recv.at[c], z, col)

    for row in range(nr):
        @pl.when(row != z)
        def _():
            mass_copy(row).start()
    for col in range(nc):
        @pl.when(col != c)
        def _():
            loss_copy(col).start()

    for j in range(m):
        @pl.when(c * m + j < z)
        def _():
            delta_copy(j).wait_send()

    def drain(g, _):
        for j in range(m):
            @pl.when(c * m + j > z)
            def _():
                run_copy(g, j).wait_send()

        @pl.when(is_owner)
        def _():
            for col in range(1, nc):
                @pl.when(col > c)
                def _():
                    core_copy(g, col).wait_send()

            @pl.when(g != z)
            def _():
                own_copy(g).wait_send()

        return 0

    lax.fori_loop(0, nr, drain, 0)

    for col in range(nc):
        @pl.when(col != c)
        def _():
            arrived(loss_all.at[col], loss_recv.at[col])
    loss_sum = loss_all[0, 0:1, :rows]
    for col in range(1, nc):
        loss_sum = loss_sum + loss_all[col, 0:1, :rows]
    loss_out[...] = loss_sum
    for row in range(nr):
        @pl.when(row != z)
        def _():
            arrived(mass_all.at[row], mass_recv.at[row])
    mass_sum = mass_all[0]
    for row in range(1, nr):
        mass_sum = mass_sum + mass_all[row]
    mass_out[...] = mass_sum

    for row in range(nr):
        @pl.when(row != z)
        def _():
            mass_copy(row).wait_send()
    for col in range(nc):
        @pl.when(col != c)
        def _():
            loss_copy(col).wait_send()


def local(nr, nc, weights, codebook, assign, chol_upper, inv_blocks):
    rows, width = weights.shape[1:]
    span = chol_upper.shape[1]
    m = width // span
    blocks, code_count = codebook.shape[1], codebook.shape[3]
    block = inv_blocks.shape[2]
    dma = pltpu.SemaphoreType.DMA
    vmem = pl.BlockSpec(memory_space=pltpu.VMEM)
    errors, loss, mass = pl.pallas_call(
        functools.partial(kernel, nr, nc),
        out_shape=(
            jax.ShapeDtypeStruct((rows, width), F32),
            jax.ShapeDtypeStruct((1, rows), F32),
            jax.ShapeDtypeStruct((blocks, code_count), F32),
        ),
        in_specs=[vmem, vmem, vmem, vmem, pl.BlockSpec(memory_space=pl.ANY)],
        out_specs=(vmem, vmem, vmem),
        scratch_shapes=[
            pltpu.VMEM((span, width), F32),
            pltpu.VMEM((span, width), BF16),
            pltpu.VMEM((span, width), BF16),
            pltpu.VMEM((span, span), F32),
            pltpu.VMEM((span, span), BF16),
            pltpu.VMEM((span, span), BF16),
            pltpu.VMEM((m, rows, span), F32),
            pltpu.VMEM((blocks, rows, block), jnp.int32),
            pltpu.VMEM((nr, rows, span), F32),
            pltpu.VMEM((nr, m, rows, span), F32),
            pltpu.VMEM((nr, m, rows, span), F32),
            pltpu.VMEM((nr, rows, span), F32),
            pltpu.VMEM((m, rows, span), F32),
            pltpu.VMEM((nr, blocks, code_count), F32),
            pltpu.VMEM((nc, 8, max(rows, 128)), F32),
            dma,
            dma((m,)), dma((nr,)),
            dma((nr, m)), dma((nr, m)),
            dma((nr, nc)), dma((nr,)),
            dma((nr,)), dma((m,)),
            dma((nr,)), dma((nr,)),
            dma((nc,)), dma((nc,)),
        ],
        compiler_params=pltpu.CompilerParams(
            collective_id=0, has_side_effects=True, vmem_limit_bytes=48 * 1024 * 1024
        ),
    )(weights[0], codebook[0], assign[0], inv_blocks[0], chol_upper[0])
    return errors[None], loss, mass[None]


def solution(mesh):
    return jax.shard_map(
        functools.partial(local, mesh.shape["row"], mesh.shape["col"]),
        mesh=mesh,
        in_specs=(
            P("ea", "row", "col"),
            P("ea", "col", None, None),
            P("ea", "row", "col"),
            P("ea", "row", "col"),
            P("ea", "col", None, None),
        ),
        out_specs=(P("ea", "row", "col"), P("ea", "row"), P("ea", "col", None)),
        check_vma=False,
    )
```

```python
import functools

import jax
import jax.numpy as jnp
from jax import lax
from jax.experimental import pallas as pl
from jax.experimental.pallas import tpu as pltpu
from jax.sharding import PartitionSpec as P

F32 = jnp.float32
BF16 = jnp.bfloat16
LOW = 16


def halves(value):
    high = value.astype(BF16)
    return high, (value - high.astype(F32)).astype(BF16)


def dot(a, b):
    return jnp.dot(a, b, preferred_element_type=F32)


def dot3(a, b_high, b_low):
    rows = a.shape[0]
    high, low = halves(a)
    both = dot(jnp.concatenate([high, low], axis=0), b_high)
    return both[:rows] + both[rows:] + dot(high, b_low)


def dot_full(a, b):
    b_high, b_low = halves(b)
    return dot3(a, b_high, b_low)


def take(table, index):
    return jnp.take_along_axis(table, index, axis=1, mode="promise_in_bounds")


def kernel(
    nr, nc,
    weights_hbm, codebook_hbm, assign_hbm, inverse_hbm, factor,
    errors_out, loss_out, mass_out,
    weights, codebook, assign, inverse, u_raw, u_high, u_low, v_full, v_high, v_low, delta, codes, delta_in, run_in, run_out,
    err_block, err_own, mass_all, loss_all,
    u_sem, d_send, d_recv, run_send, run_recv, core_send, core_recv, own_send, own_recv,
    mass_send, mass_recv, loss_send, loss_recv,
):
    z = lax.axis_index("row")
    c = lax.axis_index("col")
    rows, width = weights.shape
    span = factor.shape[0]
    m = width // span
    block = inverse.shape[1]
    k = span // block
    code_count = codebook.shape[2]
    owner = z // m
    slot = z % m
    is_owner = c == owner

    def remote(src, dst, send, recv, row, col):
        return pltpu.make_async_remote_copy(
            src_ref=src, dst_ref=dst, send_sem=send, recv_sem=recv,
            device_id={"row": row, "col": col}, device_id_type=pl.DeviceIdType.MESH,
        )

    loads = [
        pltpu.make_async_copy(source, target, u_sem.at[number])
        for number, (source, target) in enumerate((
            (assign_hbm, assign), (codebook_hbm, codebook), (weights_hbm, weights),
            (inverse_hbm, inverse), (factor, u_raw),
        ))
    ]
    for load in loads:
        load.start()

    barrier = pltpu.get_barrier_semaphore()
    for step in range(1, nr * nc):
        other = lax.rem(z * nc + c + step, nr * nc)
        pl.semaphore_signal(
            barrier, inc=1, device_id={"row": other // nc, "col": other % nc},
            device_id_type=pl.DeviceIdType.MESH,
        )

    for load in loads[:3]:
        load.wait()

    lane = lax.broadcasted_iota(jnp.int32, (rows, block), 1)
    for b in range(width // block):
        first = b * (block // 2)
        tile = first // block * block
        code = take(assign[:, tile:tile + block], first - tile + lane // 2)
        codes[b] = code
        inner = code % block
        value = jnp.zeros((rows, block), F32)
        for part in range(code_count // block):
            picked = []
            for comp in range(2):
                table = codebook[b, comp:comp + 1, part * block:(part + 1) * block]
                picked.append(take(jnp.broadcast_to(table, (rows, block)), inner))
            both = jnp.where(lane % 2 == 0, picked[0], picked[1])
            value = jnp.where(code // block == part, both, value)
        j, at = b * block // span, b * block % span
        delta[j, :, at:at + block] = weights[:, b * block:(b + 1) * block] - value

    @pl.when(z == 0)
    def _():
        run_in[...] = jnp.zeros_like(run_in)

    pl.semaphore_wait(barrier, nr * nc - 1)

    def delta_copy(j):
        return remote(delta.at[j], delta_in.at[z], d_send.at[j], d_recv.at[z], c * m + j, c)

    for j in range(m):
        @pl.when(c * m + j < z)
        def _():
            delta_copy(j).start()

    for load in loads[3:]:
        load.wait()

    @pl.when(is_owner)
    def _():
        v_full[...] = jnp.zeros_like(v_full)
        base = slot * span

        def invert(lo, hi):
            if hi - lo == 1:
                v_full[lo * block:hi * block, lo * block:hi * block] = inverse[slot * k + lo]
                return
            mid = (lo + hi) // 2
            invert(lo, mid)
            invert(mid, hi)
            top, middle, end = lo * block, mid * block, hi * block
            right = u_raw[top:middle, pl.ds(pl.multiple_of(base + middle, block), end - middle)]
            product = dot_full(v_full[top:middle, top:middle], right)
            v_full[top:middle, middle:end] = -dot_full(product, v_full[middle:end, middle:end])

        invert(0, k)
        high, low = halves(v_full[...])
        v_high[...] = high
        v_low[...] = low

    for j in range(m):
        @pl.when(c * m + j > z)
        def _():
            high, low = halves(u_raw[:, j * span:(j + 1) * span])
            u_high[:, j * span:(j + 1) * span] = high
            u_low[:, j * span:(j + 1) * span] = low

    def run_copy(g, j):
        return remote(run_out.at[g, j], run_in.at[g, j], run_send.at[g, j], run_recv.at[g, j], z + 1, c)

    def core_copy(g, col):
        return remote(err_block.at[g], err_block.at[g], core_send.at[g, col], core_recv.at[g], z, col)

    def own_copy(g):
        return remote(err_block.at[g], err_own.at[slot], own_send.at[g], own_recv.at[slot], g, c)

    def arrived(ref, sem):
        pltpu.make_async_copy(ref, ref, sem).wait()

    def stage(g, _):
        @pl.when(is_owner)
        def _():
            @pl.when(z > 0)
            def _():
                arrived(run_in.at[g, slot], run_recv.at[g, slot])

            @pl.when(g > z)
            def _():
                arrived(delta_in.at[g], d_recv.at[g])
                run_in[g, slot] = run_in[g, slot] + delta_in[g]

            @pl.when(g == z)
            def _():
                run_in[g, slot] = run_in[g, slot] + delta[slot]

            error = dot3(run_in[g, slot], v_high[...], v_low[...])
            err_block[g] = error

            @pl.when(g == z)
            def _():
                err_own[slot] = error

            for col in range(1, nc):
                @pl.when(col > c)
                def _():
                    core_copy(g, col).start()

            @pl.when(g < z)
            def _():
                own_copy(g).start()

        @pl.when(c > owner)
        def _():
            arrived(err_block.at[g], core_recv.at[g])

        for j in range(m):
            @pl.when(c * m + j > z)
            def _():
                change = dot3(
                    err_block[g], u_high[:, j * span:(j + 1) * span], u_low[:, j * span:(j + 1) * span]
                )

                @pl.when(z > 0)
                def _():
                    arrived(run_in.at[g, j], run_recv.at[g, j])

                local = jnp.where(g == z, delta[j], 0.0)
                run_out[g, j] = run_in[g, j] + local - change
                run_copy(g, j).start()

        return 0

    lax.fori_loop(0, nr, stage, 0)

    for g in range(1, nr):
        @pl.when(is_owner & (g > z))
        def _():
            own_copy(g).start()

    high_count = code_count // LOW
    group = 2 * high_count
    chunk = 8
    loss = jnp.zeros((8, rows), F32)
    for j in range(m):
        @pl.when(c * m + j != z)
        def _():
            arrived(err_own.at[j], own_recv.at[j])

        error = err_own[j]
        errors_out[:, j * span:(j + 1) * span] = error
        squared = error * error
        loss = loss + lax.dot_general(
            jnp.ones((8, span), F32), squared, (((1,), (1,)), ((), ())),
            precision=lax.Precision.HIGHEST, preferred_element_type=F32,
        )

        def gather(step, total):
            at = pl.ds(pl.multiple_of(step * chunk, chunk), chunk)
            iota_high = lax.broadcasted_iota(jnp.int32, (high_count, block), 0)
            iota_low = lax.broadcasted_iota(jnp.int32, (LOW, block), 0)
            left, right = [], []
            for b in range(k):
                code = codes[j * k + b, at, :]
                value = err_own[j, at, b * block:(b + 1) * block]
                value = value * value
                coarse = value.astype(BF16).astype(F32)
                fine = value - coarse
                code_high, code_low = code // LOW, code % LOW
                top, bottom, marks = [], [], []
                for r in range(chunk):
                    hit = jnp.broadcast_to(code_high[r:r + 1], (high_count, block)) == iota_high
                    top.append(jnp.where(hit, jnp.broadcast_to(coarse[r:r + 1], (high_count, block)), 0.0).astype(BF16))
                    bottom.append(jnp.where(hit, jnp.broadcast_to(fine[r:r + 1], (high_count, block)), 0.0).astype(BF16))
                    low_hit = jnp.broadcast_to(code_low[r:r + 1], (LOW, block)) == iota_low
                    marks.append(jnp.where(low_hit, 1.0, 0.0).astype(BF16))
                left += [jnp.concatenate(top, axis=1), jnp.concatenate(bottom, axis=1)]
                right.append(jnp.concatenate(marks, axis=1))
            return total + lax.dot_general(
                jnp.concatenate(left, axis=0), jnp.concatenate(right, axis=0),
                (((1,), (1,)), ((), ())), preferred_element_type=F32,
            )

        total = lax.fori_loop(0, rows // chunk, gather, jnp.zeros((k * group, k * LOW), F32), unroll=4)
        row_id = lax.broadcasted_iota(jnp.int32, total.shape, 0)
        col_id = lax.broadcasted_iota(jnp.int32, total.shape, 1)
        total = jnp.where(row_id // group == col_id // LOW, total, 0.0)
        wide_row = lax.broadcasted_iota(jnp.int32, (k * LOW, code_count), 0)
        wide_col = lax.broadcasted_iota(jnp.int32, (k * LOW, code_count), 1)
        spread = jnp.where(wide_row % LOW == wide_col % LOW, 1.0, 0.0)
        spread = jnp.dot(total, spread, precision=lax.Precision.HIGHEST, preferred_element_type=F32)
        out_row = lax.broadcasted_iota(jnp.int32, spread.shape, 0)
        out_col = lax.broadcasted_iota(jnp.int32, spread.shape, 1)
        spread = jnp.where(out_row % high_count == out_col // LOW, spread, 0.0)
        for b in range(k):
            mass_all[z, j * k + b:j * k + b + 1, :] = jnp.sum(
                spread[b * group:(b + 1) * group], axis=0, keepdims=True
            )

    loss_all[c, :, :rows] = loss

    def mass_copy(row):
        return remote(mass_all.at[z], mass_all.at[z], mass_send.at[row], mass_recv.at[z], row, c)

    def loss_copy(col):
        return remote(loss_all.at[c], loss_all.at[c], loss_send.at[col], loss_recv.at[c], z, col)

    for row in range(nr):
        @pl.when(row != z)
        def _():
            mass_copy(row).start()
    for col in range(nc):
        @pl.when(col != c)
        def _():
            loss_copy(col).start()

    for j in range(m):
        @pl.when(c * m + j < z)
        def _():
            delta_copy(j).wait_send()

    def drain(g, _):
        for j in range(m):
            @pl.when(c * m + j > z)
            def _():
                run_copy(g, j).wait_send()

        @pl.when(is_owner)
        def _():
            for col in range(1, nc):
                @pl.when(col > c)
                def _():
                    core_copy(g, col).wait_send()

            @pl.when(g != z)
            def _():
                own_copy(g).wait_send()

        return 0

    lax.fori_loop(0, nr, drain, 0)

    for col in range(nc):
        @pl.when(col != c)
        def _():
            arrived(loss_all.at[col], loss_recv.at[col])
    loss_sum = loss_all[0, 0:1, :rows]
    for col in range(1, nc):
        loss_sum = loss_sum + loss_all[col, 0:1, :rows]
    loss_out[...] = loss_sum
    for row in range(nr):
        @pl.when(row != z)
        def _():
            arrived(mass_all.at[row], mass_recv.at[row])
    mass_sum = mass_all[0]
    for row in range(1, nr):
        mass_sum = mass_sum + mass_all[row]
    mass_out[...] = mass_sum

    for row in range(nr):
        @pl.when(row != z)
        def _():
            mass_copy(row).wait_send()
    for col in range(nc):
        @pl.when(col != c)
        def _():
            loss_copy(col).wait_send()


def local(nr, nc, weights, codebook, assign, chol_upper, inv_blocks):
    rows, width = weights.shape[1:]
    span = chol_upper.shape[1]
    m = width // span
    blocks, code_count = codebook.shape[1], codebook.shape[3]
    block = inv_blocks.shape[2]
    dma = pltpu.SemaphoreType.DMA
    vmem = pl.BlockSpec(memory_space=pltpu.VMEM)
    errors, loss, mass = pl.pallas_call(
        functools.partial(kernel, nr, nc),
        out_shape=(
            jax.ShapeDtypeStruct((rows, width), F32),
            jax.ShapeDtypeStruct((1, rows), F32),
            jax.ShapeDtypeStruct((blocks, code_count), F32),
        ),
        in_specs=[pl.BlockSpec(memory_space=pl.ANY)] * 5,
        out_specs=(vmem, vmem, vmem),
        scratch_shapes=[
            pltpu.VMEM(weights.shape[1:], F32),
            pltpu.VMEM(codebook.shape[1:], F32),
            pltpu.VMEM(assign.shape[1:], jnp.int32),
            pltpu.VMEM(inv_blocks.shape[1:], F32),
            pltpu.VMEM((span, width), F32),
            pltpu.VMEM((span, width), BF16),
            pltpu.VMEM((span, width), BF16),
            pltpu.VMEM((span, span), F32),
            pltpu.VMEM((span, span), BF16),
            pltpu.VMEM((span, span), BF16),
            pltpu.VMEM((m, rows, span), F32),
            pltpu.VMEM((blocks, rows, block), jnp.int32),
            pltpu.VMEM((nr, rows, span), F32),
            pltpu.VMEM((nr, m, rows, span), F32),
            pltpu.VMEM((nr, m, rows, span), F32),
            pltpu.VMEM((nr, rows, span), F32),
            pltpu.VMEM((m, rows, span), F32),
            pltpu.VMEM((nr, blocks, code_count), F32),
            pltpu.VMEM((nc, 8, max(rows, 128)), F32),
            dma((5,)),
            dma((m,)), dma((nr,)),
            dma((nr, m)), dma((nr, m)),
            dma((nr, nc)), dma((nr,)),
            dma((nr,)), dma((m,)),
            dma((nr,)), dma((nr,)),
            dma((nc,)), dma((nc,)),
        ],
        compiler_params=pltpu.CompilerParams(
            collective_id=0, has_side_effects=True, vmem_limit_bytes=62 * 1024 * 1024
        ),
    )(weights[0], codebook[0], assign[0], inv_blocks[0], chol_upper[0])
    return errors[None], loss, mass[None]


def solution(mesh):
    return jax.shard_map(
        functools.partial(local, mesh.shape["row"], mesh.shape["col"]),
        mesh=mesh,
        in_specs=(
            P("ea", "row", "col"),
            P("ea", "col", None, None),
            P("ea", "row", "col"),
            P("ea", "row", "col"),
            P("ea", "col", None, None),
        ),
        out_specs=(P("ea", "row", "col"), P("ea", "row"), P("ea", "col", None)),
        check_vma=False,
    )
```

```python
import functools

import jax
import jax.numpy as jnp
from jax import lax
from jax.experimental import pallas as pl
from jax.experimental.pallas import tpu as pltpu
from jax.sharding import PartitionSpec as P

F32 = jnp.float32
BF16 = jnp.bfloat16
LOW = 16
PIECES = 2


def halves(value):
    high = value.astype(BF16)
    return high, (value - high.astype(F32)).astype(BF16)


def dot(a, b):
    return jnp.dot(a, b, preferred_element_type=F32)


def dot3(a, b_high, b_low):
    rows = a.shape[0]
    high, low = halves(a)
    both = dot(jnp.concatenate([high, low], axis=0), b_high)
    return both[:rows] + both[rows:] + dot(high, b_low)


def dot_full(a, b):
    b_high, b_low = halves(b)
    return dot3(a, b_high, b_low)


def take(table, index):
    return jnp.take_along_axis(table, index, axis=1, mode="promise_in_bounds")


def kernel(
    nr, nc,
    weights_hbm, codebook_hbm, assign_hbm, inverse_hbm, factor,
    errors_out, loss_out, mass_out,
    weights, codebook, assign, inverse, u_raw, u_high, u_low, v_full, v_high, v_low, delta, codes, delta_in, run_in, run_out,
    err_block, err_own, mass_all, loss_all,
    u_sem, d_send, d_recv, run_send, run_recv, core_send, core_recv, own_send, own_recv,
    mass_send, mass_recv, loss_send, loss_recv,
):
    z = lax.axis_index("row")
    c = lax.axis_index("col")
    rows, width = weights.shape
    span = factor.shape[0]
    m = width // span
    block = inverse.shape[1]
    k = span // block
    code_count = codebook.shape[2]
    owner = z // m
    slot = z % m
    steps = nr * PIECES
    piece = rows // PIECES
    is_owner = c == owner

    def remote(src, dst, send, recv, row, col):
        return pltpu.make_async_remote_copy(
            src_ref=src, dst_ref=dst, send_sem=send, recv_sem=recv,
            device_id={"row": row, "col": col}, device_id_type=pl.DeviceIdType.MESH,
        )

    loads = [
        pltpu.make_async_copy(source, target, u_sem.at[number])
        for number, (source, target) in enumerate((
            (assign_hbm, assign), (codebook_hbm, codebook), (weights_hbm, weights),
            (inverse_hbm, inverse), (factor, u_raw),
        ))
    ]
    for load in loads:
        load.start()

    barrier = pltpu.get_barrier_semaphore()
    for step in range(1, nr * nc):
        other = lax.rem(z * nc + c + step, nr * nc)
        pl.semaphore_signal(
            barrier, inc=1, device_id={"row": other // nc, "col": other % nc},
            device_id_type=pl.DeviceIdType.MESH,
        )

    for load in loads[:3]:
        load.wait()

    lane = lax.broadcasted_iota(jnp.int32, (rows, block), 1)
    for b in range(width // block):
        first = b * (block // 2)
        tile = first // block * block
        code = take(assign[:, tile:tile + block], first - tile + lane // 2)
        codes[b] = code
        inner = code % block
        value = jnp.zeros((rows, block), F32)
        for part in range(code_count // block):
            picked = []
            for comp in range(2):
                table = codebook[b, comp:comp + 1, part * block:(part + 1) * block]
                picked.append(take(jnp.broadcast_to(table, (rows, block)), inner))
            both = jnp.where(lane % 2 == 0, picked[0], picked[1])
            value = jnp.where(code // block == part, both, value)
        j, at = b * block // span, b * block % span
        delta[j, :, at:at + block] = weights[:, b * block:(b + 1) * block] - value

    @pl.when(z == 0)
    def _():
        run_in[...] = jnp.zeros_like(run_in)

    pl.semaphore_wait(barrier, nr * nc - 1)

    def delta_copy(j):
        return remote(delta.at[j], delta_in.at[z], d_send.at[j], d_recv.at[z], c * m + j, c)

    for j in range(m):
        @pl.when(c * m + j < z)
        def _():
            delta_copy(j).start()

    for load in loads[3:]:
        load.wait()

    @pl.when(is_owner)
    def _():
        v_full[...] = jnp.zeros_like(v_full)
        base = slot * span

        def invert(lo, hi):
            if hi - lo == 1:
                v_full[lo * block:hi * block, lo * block:hi * block] = inverse[slot * k + lo]
                return
            mid = (lo + hi) // 2
            invert(lo, mid)
            invert(mid, hi)
            top, middle, end = lo * block, mid * block, hi * block
            right = u_raw[top:middle, pl.ds(pl.multiple_of(base + middle, block), end - middle)]
            product = dot_full(v_full[top:middle, top:middle], right)
            v_full[top:middle, middle:end] = -dot_full(product, v_full[middle:end, middle:end])

        invert(0, k)
        high, low = halves(v_full[...])
        v_high[...] = high
        v_low[...] = low

    for j in range(m):
        @pl.when(c * m + j > z)
        def _():
            high, low = halves(u_raw[:, j * span:(j + 1) * span])
            u_high[:, j * span:(j + 1) * span] = high
            u_low[:, j * span:(j + 1) * span] = low

    def run_copy(g, j):
        return remote(run_out.at[g, j], run_in.at[g, j], run_send.at[g, j], run_recv.at[g, j], z + 1, c)

    def core_copy(g, col):
        return remote(err_block.at[g], err_block.at[g], core_send.at[g, col], core_recv.at[g], z, col)

    def part_rows(q):
        return pl.ds(pl.multiple_of(q % PIECES * piece, piece), piece)

    def own_copy(q):
        return remote(
            err_block.at[q], err_own.at[slot, part_rows(q)],
            own_send.at[q], own_recv.at[slot, q % PIECES], q // PIECES, c,
        )

    def arrived(ref, sem):
        pltpu.make_async_copy(ref, ref, sem).wait()

    def stage(q, _):
        g = q // PIECES
        at = part_rows(q)

        @pl.when(is_owner)
        def _():
            @pl.when(z > 0)
            def _():
                arrived(run_in.at[q, slot], run_recv.at[q, slot])

            @pl.when(g > z)
            def _():
                @pl.when(q % PIECES == 0)
                def _():
                    arrived(delta_in.at[g], d_recv.at[g])

                run_in[q, slot] = run_in[q, slot] + delta_in[g, at]

            @pl.when(g == z)
            def _():
                run_in[q, slot] = run_in[q, slot] + delta[slot, at]

            error = dot3(run_in[q, slot], v_high[...], v_low[...])
            err_block[q] = error

            @pl.when(g == z)
            def _():
                err_own[slot, at] = error

            for col in range(1, nc):
                @pl.when(col > c)
                def _():
                    core_copy(q, col).start()

            @pl.when(g < z)
            def _():
                own_copy(q).start()

        @pl.when(c > owner)
        def _():
            arrived(err_block.at[q], core_recv.at[q])

        for j in range(m):
            @pl.when(c * m + j > z)
            def _():
                change = dot3(
                    err_block[q], u_high[:, j * span:(j + 1) * span], u_low[:, j * span:(j + 1) * span]
                )

                @pl.when(z > 0)
                def _():
                    arrived(run_in.at[q, j], run_recv.at[q, j])

                local = jnp.where(g == z, delta[j, at], 0.0)
                run_out[q, j] = run_in[q, j] + local - change
                run_copy(q, j).start()

        return 0

    lax.fori_loop(0, steps, stage, 0)

    for q in range(PIECES, steps):
        @pl.when(is_owner & (q // PIECES > z))
        def _():
            own_copy(q).start()

    high_count = code_count // LOW
    group = 2 * high_count
    chunk = 8
    loss = jnp.zeros((8, rows), F32)
    for j in range(m):
        @pl.when(c * m + j != z)
        def _():
            for h in range(PIECES):
                arrived(err_own.at[j, h * piece:(h + 1) * piece], own_recv.at[j, h])

        error = err_own[j]
        errors_out[:, j * span:(j + 1) * span] = error
        squared = error * error
        loss = loss + lax.dot_general(
            jnp.ones((8, span), F32), squared, (((1,), (1,)), ((), ())),
            precision=lax.Precision.HIGHEST, preferred_element_type=F32,
        )

        def gather(step, total):
            at = pl.ds(pl.multiple_of(step * chunk, chunk), chunk)
            iota_high = lax.broadcasted_iota(jnp.int32, (high_count, block), 0)
            iota_low = lax.broadcasted_iota(jnp.int32, (LOW, block), 0)
            left, right = [], []
            for b in range(k):
                code = codes[j * k + b, at, :]
                value = err_own[j, at, b * block:(b + 1) * block]
                value = value * value
                coarse = value.astype(BF16).astype(F32)
                fine = value - coarse
                code_high, code_low = code // LOW, code % LOW
                top, bottom, marks = [], [], []
                for r in range(chunk):
                    hit = jnp.broadcast_to(code_high[r:r + 1], (high_count, block)) == iota_high
                    top.append(jnp.where(hit, jnp.broadcast_to(coarse[r:r + 1], (high_count, block)), 0.0).astype(BF16))
                    bottom.append(jnp.where(hit, jnp.broadcast_to(fine[r:r + 1], (high_count, block)), 0.0).astype(BF16))
                    low_hit = jnp.broadcast_to(code_low[r:r + 1], (LOW, block)) == iota_low
                    marks.append(jnp.where(low_hit, 1.0, 0.0).astype(BF16))
                left += [jnp.concatenate(top, axis=1), jnp.concatenate(bottom, axis=1)]
                right.append(jnp.concatenate(marks, axis=1))
            return total + lax.dot_general(
                jnp.concatenate(left, axis=0), jnp.concatenate(right, axis=0),
                (((1,), (1,)), ((), ())), preferred_element_type=F32,
            )

        total = lax.fori_loop(0, rows // chunk, gather, jnp.zeros((k * group, k * LOW), F32), unroll=4)
        row_id = lax.broadcasted_iota(jnp.int32, total.shape, 0)
        col_id = lax.broadcasted_iota(jnp.int32, total.shape, 1)
        total = jnp.where(row_id // group == col_id // LOW, total, 0.0)
        wide_row = lax.broadcasted_iota(jnp.int32, (k * LOW, code_count), 0)
        wide_col = lax.broadcasted_iota(jnp.int32, (k * LOW, code_count), 1)
        spread = jnp.where(wide_row % LOW == wide_col % LOW, 1.0, 0.0)
        spread = jnp.dot(total, spread, precision=lax.Precision.HIGHEST, preferred_element_type=F32)
        out_row = lax.broadcasted_iota(jnp.int32, spread.shape, 0)
        out_col = lax.broadcasted_iota(jnp.int32, spread.shape, 1)
        spread = jnp.where(out_row % high_count == out_col // LOW, spread, 0.0)
        for b in range(k):
            mass_all[z, j * k + b:j * k + b + 1, :] = jnp.sum(
                spread[b * group:(b + 1) * group], axis=0, keepdims=True
            )

    loss_all[c, :, :rows] = loss

    def mass_copy(row):
        return remote(mass_all.at[z], mass_all.at[z], mass_send.at[row], mass_recv.at[z], row, c)

    def loss_copy(col):
        return remote(loss_all.at[c], loss_all.at[c], loss_send.at[col], loss_recv.at[c], z, col)

    for row in range(nr):
        @pl.when(row != z)
        def _():
            mass_copy(row).start()
    for col in range(nc):
        @pl.when(col != c)
        def _():
            loss_copy(col).start()

    for j in range(m):
        @pl.when(c * m + j < z)
        def _():
            delta_copy(j).wait_send()

    def drain(q, _):
        for j in range(m):
            @pl.when(c * m + j > z)
            def _():
                run_copy(q, j).wait_send()

        @pl.when(is_owner)
        def _():
            for col in range(1, nc):
                @pl.when(col > c)
                def _():
                    core_copy(q, col).wait_send()

            @pl.when(q // PIECES != z)
            def _():
                own_copy(q).wait_send()

        return 0

    lax.fori_loop(0, steps, drain, 0)

    for col in range(nc):
        @pl.when(col != c)
        def _():
            arrived(loss_all.at[col], loss_recv.at[col])
    loss_sum = loss_all[0, 0:1, :rows]
    for col in range(1, nc):
        loss_sum = loss_sum + loss_all[col, 0:1, :rows]
    loss_out[...] = loss_sum
    for row in range(nr):
        @pl.when(row != z)
        def _():
            arrived(mass_all.at[row], mass_recv.at[row])
    mass_sum = mass_all[0]
    for row in range(1, nr):
        mass_sum = mass_sum + mass_all[row]
    mass_out[...] = mass_sum

    for row in range(nr):
        @pl.when(row != z)
        def _():
            mass_copy(row).wait_send()
    for col in range(nc):
        @pl.when(col != c)
        def _():
            loss_copy(col).wait_send()


def local(nr, nc, weights, codebook, assign, chol_upper, inv_blocks):
    rows, width = weights.shape[1:]
    span = chol_upper.shape[1]
    m = width // span
    steps, piece = nr * PIECES, rows // PIECES
    blocks, code_count = codebook.shape[1], codebook.shape[3]
    block = inv_blocks.shape[2]
    dma = pltpu.SemaphoreType.DMA
    vmem = pl.BlockSpec(memory_space=pltpu.VMEM)
    errors, loss, mass = pl.pallas_call(
        functools.partial(kernel, nr, nc),
        out_shape=(
            jax.ShapeDtypeStruct((rows, width), F32),
            jax.ShapeDtypeStruct((1, rows), F32),
            jax.ShapeDtypeStruct((blocks, code_count), F32),
        ),
        in_specs=[pl.BlockSpec(memory_space=pl.ANY)] * 5,
        out_specs=(vmem, vmem, vmem),
        scratch_shapes=[
            pltpu.VMEM(weights.shape[1:], F32),
            pltpu.VMEM(codebook.shape[1:], F32),
            pltpu.VMEM(assign.shape[1:], jnp.int32),
            pltpu.VMEM(inv_blocks.shape[1:], F32),
            pltpu.VMEM((span, width), F32),
            pltpu.VMEM((span, width), BF16),
            pltpu.VMEM((span, width), BF16),
            pltpu.VMEM((span, span), F32),
            pltpu.VMEM((span, span), BF16),
            pltpu.VMEM((span, span), BF16),
            pltpu.VMEM((m, rows, span), F32),
            pltpu.VMEM((blocks, rows, block), jnp.int32),
            pltpu.VMEM((nr, rows, span), F32),
            pltpu.VMEM((steps, m, piece, span), F32),
            pltpu.VMEM((steps, m, piece, span), F32),
            pltpu.VMEM((steps, piece, span), F32),
            pltpu.VMEM((m, rows, span), F32),
            pltpu.VMEM((nr, blocks, code_count), F32),
            pltpu.VMEM((nc, 8, max(rows, 128)), F32),
            dma((5,)),
            dma((m,)), dma((nr,)),
            dma((steps, m)), dma((steps, m)),
            dma((steps, nc)), dma((steps,)),
            dma((steps,)), dma((m, PIECES)),
            dma((nr,)), dma((nr,)),
            dma((nc,)), dma((nc,)),
        ],
        compiler_params=pltpu.CompilerParams(
            collective_id=0, has_side_effects=True, vmem_limit_bytes=62 * 1024 * 1024
        ),
    )(weights[0], codebook[0], assign[0], inv_blocks[0], chol_upper[0])
    return errors[None], loss, mass[None]


def solution(mesh):
    return jax.shard_map(
        functools.partial(local, mesh.shape["row"], mesh.shape["col"]),
        mesh=mesh,
        in_specs=(
            P("ea", "row", "col"),
            P("ea", "col", None, None),
            P("ea", "row", "col"),
            P("ea", "row", "col"),
            P("ea", "col", None, None),
        ),
        out_specs=(P("ea", "row", "col"), P("ea", "row"), P("ea", "col", None)),
        check_vma=False,
    )
```
